32 devices in a mesh: row: 4 (over y, core), col: 8 (over z, x).
Axes of the slice: x: 2, y: 2, z: 4, core: 2. Of those that a mesh axis runs over, the one named last changes fastest.
Arguments:
- out_weights: bfloat16 [2048, 2048], P('row', 'col'), may hold values from -1 to 1
- in_weights: bfloat16 [2048, 2048], P('row', 'col'), may hold values from -1 to 1, as said below
- tile_list: int32 [16, 12], replicated, may hold values from 0 to 15, as said below
- tile_count: int32 [16], replicated, may hold values from 1 to 12, as said below
- owner: int32 [16], replicated, may hold values from 0 to 3, as said below
Outputs:
- transitive: float32 [2048], P('row')
- cyclic: float32 [2048], P('row')
The draws below stay inside these ranges and needn't reach their ends.
Inputs may be any that keep to these rules, and one draw needn't show every extreme that they name: in_weights is the transpose of out_weights. `tile_list`: the 12 entries of a row are distinct tile columns. Only the first tile_count[a] entries of row a of tile_list are live. `owner`: each index of row owns exactly 4 tile rows, and at most 1 of the tile rows s * 4 to (s + 1) * 4 - 1, for every s; tile row t is owned by the index (t // 4 + e) mod 4 for some e from 0 to 3.
All inputs are finite; a program needn't handle non-finite values.
Results may differ from the reference program's by a relative error of at most 0.0003.
Values may be sent and summed in bfloat16 or wider, within the bound.
A program may use at most 64 MiB of HBM per device.

```python
import jax
import jax.numpy as jnp

TILE = 128
N = 2048
NT = 16
TILE_ROWS = 4
KMAX = 12


def graph_values(key):
    base_key = jax.random.fold_in(key, 11)
    key_values = jax.random.fold_in(base_key, 0)
    spread = TILE ** (-0.5)
    values = jnp.clip(jax.random.normal(key_values, (N, N), jnp.float32), -4.0, 4.0)
    return values * spread


def draw_out_weights(key, part):
    return graph_values(key).astype(jnp.bfloat16)


def draw_in_weights(key, part):
    return graph_values(key).T.astype(jnp.bfloat16)


def draw_tile_list(key, part):
    scores = jax.random.randint(jax.random.fold_in(key, 23), (NT, NT), 0, 1 << 20) * NT + jnp.arange(NT, dtype=jnp.int32)[None, :]
    return jnp.argsort(scores, axis=1, stable=True)[:, :KMAX].astype(jnp.int32)


def draw_tile_count(key, part):
    subkeys = jax.random.split(jax.random.fold_in(key, 37), 3)
    dense_row = jax.random.randint(subkeys[0], (NT,), 0, 2)
    lowest = jnp.where(dense_row == 1, KMAX // 2, KMAX // 4)
    highest = jnp.where(dense_row == 1, KMAX, KMAX // 2)
    counts = lowest + jax.random.randint(subkeys[1], (NT,), 0, 1 << 20) % (highest - lowest + 1)
    chosen = jax.random.randint(subkeys[2], (), 0, NT)
    return counts.at[chosen].set(KMAX).astype(jnp.int32)


def draw_owner(key, part):
    groups = NT // TILE_ROWS
    scores = jax.random.randint(jax.random.fold_in(key, 41), (groups, TILE_ROWS), 0, 1 << 20) * TILE_ROWS + jnp.arange(TILE_ROWS, dtype=jnp.int32)[None, :]
    offsets = jnp.argsort(scores, axis=1, stable=True).astype(jnp.int32)
    source = jnp.arange(NT, dtype=jnp.int32) // TILE_ROWS
    within = jnp.arange(NT, dtype=jnp.int32) % TILE_ROWS
    return ((source + offsets[source, within]) % groups).astype(jnp.int32)


def setup_inputs(seed: int = 0) -> dict:
    arg_keys = jax.random.split(jax.random.key(seed), 6)
    out_weights = draw_out_weights(jax.random.fold_in(arg_keys[5], 71), 0)
    in_weights = draw_in_weights(jax.random.fold_in(arg_keys[5], 71), 0)
    tile_list = draw_tile_list(jax.random.fold_in(arg_keys[5], 71), 0)
    tile_count = draw_tile_count(jax.random.fold_in(arg_keys[5], 71), 0)
    owner = draw_owner(jax.random.fold_in(arg_keys[5], 71), 0)
    return dict(out_weights=out_weights, in_weights=in_weights, tile_list=tile_list, tile_count=tile_count, owner=owner)


def tile_mask(tile_list, tile_count):
    live_slots = jnp.arange(tile_list.shape[1], dtype=jnp.int32)[None, :] < tile_count[:, None]
    matches = (tile_list[:, :, None] == jnp.arange(NT, dtype=jnp.int32)[None, None, :]) & live_slots[:, :, None]
    return jnp.any(matches, axis=1)


def spread_tiles(listed):
    return jnp.repeat(jnp.repeat(listed, TILE, axis=0), TILE, axis=1)


def reference(out_weights, in_weights, tile_list, tile_count, owner):
    listed = tile_mask(tile_list, tile_count)
    out_eff = jnp.where(spread_tiles(listed), out_weights, jnp.zeros_like(out_weights))
    in_eff = jnp.where(spread_tiles(listed.T), in_weights, jnp.zeros_like(in_weights))
    two_paths = jnp.dot(out_eff, out_eff, preferred_element_type=jnp.float32)
    trans_all = jnp.sum(out_eff.astype(jnp.float32) * two_paths, axis=1)
    cyc_all = jnp.sum(in_eff.astype(jnp.float32) * two_paths, axis=1)
    owner_order = jnp.argsort(owner, stable=True).astype(jnp.int32)
    node_order = (owner_order[:, None] * TILE + jnp.arange(TILE, dtype=jnp.int32)[None, :]).reshape(-1)
    return trans_all[node_order], cyc_all[node_order]
```

```python
import functools

import jax
import jax.numpy as jnp
from jax import lax
from jax.experimental import pallas as pl
from jax.experimental.pallas import tpu as pltpu
from jax.sharding import PartitionSpec as P

TILE = 128
HALVES = 2
MESH = pl.DeviceIdType.MESH


def kernel(rows_n, cols_n, out_ref, in_ref, list_ref, count_ref, owner_ref, trans_ref, cyc_ref,
           own, colp, rowp, inb, mask, acc, sendbuf, recvbuf,
           load_sem, local_sem, swap_send, swap_recv, col_send, col_recv, in_send, in_recv,
           up_send, dn_send, sib_send, row_recv, res_send, res_recv):
    rb, cb = out_ref.shape
    tr, ct = rb // TILE, cb // TILE
    nt, slots = list_ref.shape
    lines = cols_n // 2
    reach = sendbuf.shape[0]
    hb = rb // HALVES
    me_r, me_c = lax.axis_index("row"), lax.axis_index("col")
    yy, p = me_r // 2, me_r % 2
    zz, a = me_c // 2, me_c % 2
    vr, vc = 2 * yy + a, 2 * zz + p

    def home(r, c):
        return (2 * (r // 2) + c % 2, 2 * (c // 2) + r % 2)

    load = pltpu.make_async_copy(out_ref, own, load_sem)
    load.start()

    barrier = pltpu.get_barrier_semaphore()

    def greet(i, carry):
        there = (me_r + i // cols_n) % rows_n, (me_c + i % cols_n) % cols_n
        pl.semaphore_signal(barrier, inc=1, device_id=there, device_id_type=MESH)
        return carry

    lax.fori_loop(1, rows_n * cols_n, greet, 0)
    load.wait()
    pl.semaphore_wait(barrier, rows_n * cols_n - 1)

    def half(h):
        return pl.ds(h * hb, hb)

    def col_at(group, h):
        return pl.ds(pl.multiple_of(group * rb + h * hb, hb), hb)

    swap = home(me_r, me_c)
    swaps = [
        pltpu.make_async_remote_copy(
            src_ref=own.at[half(h)], dst_ref=colp.at[col_at(me_r, h)], send_sem=swap_send.at[h],
            recv_sem=swap_recv.at[h], device_id=swap, device_id_type=MESH)
        for h in range(HALVES)
    ]
    swaps_here = [
        pltpu.make_async_copy(own.at[half(h)], colp.at[col_at(me_r, h)], swap_recv.at[h])
        for h in range(HALVES)
    ]
    give_in = pltpu.make_async_remote_copy(
        src_ref=in_ref, dst_ref=inb, send_sem=in_send, recv_sem=in_recv, device_id=swap, device_id_type=MESH)
    keep_in = pltpu.make_async_copy(in_ref, inb, in_recv)

    def col_copy(s):
        return pltpu.make_async_remote_copy(
            src_ref=own, dst_ref=colp.at[pl.ds(pl.multiple_of(me_r * rb, rb), rb)],
            send_sem=col_send.at[s], recv_sem=col_recv.at[s],
            device_id=home((me_r + s) % rows_n, me_c), device_id_type=MESH)

    @pl.when(a == p)
    def _():
        for h in range(HALVES):
            swaps_here[h].start()
        keep_in.start()

    @pl.when(a != p)
    def _():
        for h in range(HALVES):
            swaps[h].start()

    def up(slot, h, src):
        return pltpu.make_async_remote_copy(
            src_ref=src, dst_ref=rowp.at[slot, half(h)], send_sem=up_send.at[slot, h],
            recv_sem=row_recv.at[slot, h], device_id=(me_r, me_c + 2), device_id_type=MESH)

    def down(slot, h, src):
        return pltpu.make_async_remote_copy(
            src_ref=src, dst_ref=rowp.at[slot, half(h)], send_sem=dn_send.at[slot, h],
            recv_sem=row_recv.at[slot, h], device_id=(me_r, me_c - 2), device_id_type=MESH)

    def sib(slot, h, src):
        return pltpu.make_async_remote_copy(
            src_ref=src, dst_ref=rowp.at[slot, half(h)], send_sem=sib_send.at[slot, h],
            recv_sem=row_recv.at[slot, h], device_id=(2 * yy + 1 - p, me_c), device_id_type=MESH)

    def wait_row(slot, h):
        pltpu.make_async_copy(rowp.at[slot, half(h)], rowp.at[slot, half(h)], row_recv.at[slot, h]).wait()

    for h in range(HALVES):
        pltpu.make_async_copy(own.at[half(h)], colp.at[col_at(vr, h)], swap_recv.at[h]).wait()
        src = colp.at[col_at(vr, h)]

        @pl.when(zz < lines - 1)
        def _():
            up(vc, h, src).start()

        @pl.when(zz > 0)
        def _():
            down(vc, h, src).start()

        sib(vc, h, src).start()
        if h == 0:
            lax.fori_loop(1, rows_n, lambda s, c: (col_copy(s).start(), c)[1], 0)

            @pl.when(a != p)
            def _():
                give_in.start()

    row_ids = lax.broadcasted_iota(jnp.int32, (nt, TILE), 0)
    lane_ids = lax.broadcasted_iota(jnp.int32, (nt, TILE), 1)
    counts = lax.fori_loop(
        0, nt, lambda t, c: jnp.where(row_ids == t, count_ref[t], c), jnp.zeros((nt, TILE), jnp.int32))
    small = jnp.zeros((nt, TILE), jnp.float32)
    for s in range(slots):
        hit = (list_ref[:, s:s + 1] == lane_ids) & (counts > s)
        small = jnp.where(hit, 1.0, small)

    def spread(t, carry):
        one = jnp.sum(jnp.where(lane_ids == t, small, 0.0), axis=1, keepdims=True)
        mask[t] = jnp.broadcast_to(one, (nt, TILE))
        return carry

    lax.fori_loop(0, nt, spread, 0)

    def forward(d):
        for h in range(HALVES):
            low, high = 2 * (zz - d) + p, 2 * (zz + d) + p

            @pl.when(zz - d >= 0)
            def _():
                wait_row(low, h)

                @pl.when(zz < lines - 1)
                def _():
                    up(low, h, rowp.at[low, half(h)]).start()

                sib(low, h, rowp.at[low, half(h)]).start()

            @pl.when(zz + d < lines)
            def _():
                wait_row(high, h)

                @pl.when(zz > 0)
                def _():
                    down(high, h, rowp.at[high, half(h)]).start()

                sib(high, h, rowp.at[high, half(h)]).start()

    def keep_of(tile, column):
        wide = [mask[column * ct + j, pl.ds(tile, 1), :] for j in range(ct)]
        return jnp.concatenate(wide, axis=1)

    def tiles(block, first_tile, column):
        parts = []
        for t in range(block.shape[0] // TILE):
            keep = keep_of(first_tile + t, column)
            parts.append(block[t * TILE:(t + 1) * TILE] * keep.astype(jnp.bfloat16))
        return jnp.concatenate(parts, axis=0)

    def product(slot, lhs):
        left = tiles(lhs, tr * vr, slot)
        right = tiles(colp[pl.ds(pl.multiple_of(slot * cb, cb), cb), :], ct * slot, vc)
        return jnp.dot(left, right, preferred_element_type=jnp.float32)

    def add(slot):
        acc[...] += product(slot, rowp[slot])

    def take(d):
        @pl.when(zz - d >= 0)
        def _():
            add(2 * (zz - d) + p)
            for h in range(HALVES):
                wait_row(2 * (zz - d) + 1 - p, h)
            add(2 * (zz - d) + 1 - p)

        @pl.when(zz + d < lines)
        def _():
            add(2 * (zz + d) + p)
            for h in range(HALVES):
                wait_row(2 * (zz + d) + 1 - p, h)
            add(2 * (zz + d) + 1 - p)

    lax.fori_loop(1, lines - 1, lambda d, c: (forward(d), c)[1], 0)

    def wait_col(s, carry):
        here = colp.at[pl.ds(pl.multiple_of((vr + rows_n - s) % rows_n * rb, rb), rb)]
        pltpu.make_async_copy(here, here, col_recv.at[s]).wait()
        return carry

    lax.fori_loop(1, rows_n, wait_col, 0)
    keep_in.wait()
    own_rows = pl.ds(pl.multiple_of(vr * rb, rb), rb)
    acc[...] = product(vc, colp[own_rows, :])
    for h in range(HALVES):
        wait_row(2 * zz + 1 - p, h)
    add(2 * zz + 1 - p)
    lax.fori_loop(1, lines - 1, lambda d, c: (take(d), c)[1], 0)
    forward(lines - 1)
    take(lines - 1)

    lefts, rights = [], []
    for q in range(tr):
        at = pl.ds(pl.multiple_of(vr * rb + q * TILE, TILE), TILE)
        total = acc[q * TILE:(q + 1) * TILE, :]
        keep = keep_of(tr * vr + q, vc)
        t_prod = colp[at, :].astype(jnp.float32) * keep * total
        t_sum, c_sum = 0.0, 0.0
        for j in range(ct):
            cols = slice(j * TILE, (j + 1) * TILE)
            keep_in_tile = mask[tr * vr + q, pl.ds(ct * vc + j, 1), :]
            t_sum += t_prod[:, cols]
            c_sum += inb[q * TILE:(q + 1) * TILE, cols].astype(jnp.float32) * keep_in_tile * total[:, cols]
        lefts.append(jnp.sum(t_sum.T, axis=0, keepdims=True))
        rights.append(jnp.sum(c_sum.T, axis=0, keepdims=True))
    for e in range(reach):
        dest = (vr + e) % rows_n
        t_out, c_out = jnp.zeros((1, TILE), jnp.float32), jnp.zeros((1, TILE), jnp.float32)
        for q in range(tr):
            mine = owner_ref[tr * vr + q] == dest
            t_out = jnp.where(mine, lefts[q], t_out)
            c_out = jnp.where(mine, rights[q], c_out)
        sendbuf[e, 0:1, :] = t_out
        sendbuf[e, 1:2, :] = c_out

    def result(e, i):
        return pltpu.make_async_remote_copy(
            src_ref=sendbuf.at[e], dst_ref=recvbuf.at[e, vc], send_sem=res_send.at[e, i],
            recv_sem=res_recv, device_id=((vr + e) % rows_n, (me_c + i) % cols_n), device_id_type=MESH)

    def each_result(act, act_here):
        for e in range(reach):
            def one(i, carry, e=e):
                here = ((vr + e) % rows_n == me_r) & (i == 0)
                pl.when(jnp.logical_not(here))(lambda: act(result(e, i)))
                return carry

            lax.fori_loop(0, cols_n, one, 0)
            if act_here:
                @pl.when((vr + e) % rows_n == me_r)
                def _():
                    pltpu.make_async_copy(sendbuf.at[e], recvbuf.at[e, vc], res_recv).start()

    each_result(lambda c: c.start(), True)

    @pl.when(a != p)
    def _():
        for h in range(HALVES):
            swaps[h].wait_send()
        give_in.wait_send()

    lax.fori_loop(1, rows_n, lambda s, c: (col_copy(s).wait_send(), c)[1], 0)

    def drain(d, carry):
        for h in range(HALVES):
            low, high = 2 * (zz - d) + p, 2 * (zz + d) + p

            @pl.when(zz - d >= 0)
            def _():
                @pl.when(zz < lines - 1)
                def _():
                    up(low, h, rowp.at[low, half(h)]).wait_send()

                sib(low, h, rowp.at[low, half(h)]).wait_send()

            @pl.when(zz + d < lines)
            def _():
                @pl.when(zz > 0)
                def _():
                    down(high, h, rowp.at[high, half(h)]).wait_send()

                @pl.when(d > 0)
                def _():
                    sib(high, h, rowp.at[high, half(h)]).wait_send()
        return carry

    lax.fori_loop(0, lines, drain, 0)
    each_result(lambda c: c.wait_send(), False)

    pltpu.make_async_copy(recvbuf, recvbuf, res_recv).wait()
    for e in range(reach):
        group = (me_r + rows_n - e) % rows_n
        place = 0
        for other in range(reach):
            place += ((me_r + rows_n - other) % rows_n < group).astype(jnp.int32)
        both = jnp.sum(recvbuf[e], axis=0)
        trans_ref[pl.ds(place, 1), :] = both[0:1, :]
        cyc_ref[pl.ds(place, 1), :] = both[1:2, :]


def solution(mesh):
    rows_n, cols_n = mesh.shape["row"], mesh.shape["col"]

    def per_device(out_weights, in_weights, tile_list, tile_count, owner):
        rb, cb = out_weights.shape
        nt = tile_list.shape[0]
        tr = rb // TILE
        lines = cols_n // 2
        assert rows_n % 2 == 0 and cols_n % 2 == 0 and tr <= rows_n
        n = rows_n * rb
        block = pltpu.VMEM((rb, cb), out_weights.dtype)
        dma = pltpu.SemaphoreType.DMA
        any_space = pl.BlockSpec(memory_space=pl.ANY)
        vmem = pl.BlockSpec(memory_space=pltpu.VMEM)
        smem = pl.BlockSpec(memory_space=pltpu.SMEM)
        trans, cyc = pl.pallas_call(
            functools.partial(kernel, rows_n, cols_n),
            out_shape=[jax.ShapeDtypeStruct((tr, TILE), jnp.float32)] * 2,
            in_specs=[any_space, any_space, vmem, smem, smem],
            out_specs=[vmem, vmem],
            scratch_shapes=[
                block,
                pltpu.VMEM((n, cb), out_weights.dtype),
                pltpu.VMEM((cols_n, rb, cb), out_weights.dtype),
                block,
                pltpu.VMEM((nt, nt, TILE), jnp.float32),
                pltpu.VMEM((rb, cb), jnp.float32),
                pltpu.VMEM((tr, 2, TILE), jnp.float32),
                pltpu.VMEM((tr, cols_n, 2, TILE), jnp.float32),
                dma, dma,
                dma((HALVES,)), dma((HALVES,)),
                dma((rows_n,)), dma((rows_n,)),
                dma, dma,
                dma((cols_n, HALVES)), dma((cols_n, HALVES)), dma((cols_n, HALVES)), dma((cols_n, HALVES)),
                dma((tr, cols_n)), dma,
            ],
            compiler_params=pltpu.CompilerParams(collective_id=0, has_side_effects=True),
            name="census",
        )(out_weights, in_weights, tile_list, tile_count, owner)
        return trans.reshape(rb), cyc.reshape(rb)

    return jax.shard_map(
        per_device, mesh=mesh,
        in_specs=(P("row", "col"), P("row", "col"), P(), P(), P()),
        out_specs=(P("row"), P("row")), check_vma=False)
```

```python
import functools

import jax
import jax.numpy as jnp
from jax import lax
from jax.experimental import pallas as pl
from jax.experimental.pallas import tpu as pltpu
from jax.sharding import PartitionSpec as P

TILE = 128
HALVES = 2
MESH = pl.DeviceIdType.MESH


def kernel(rows_n, cols_n, out_ref, in_ref, list_ref, count_ref, owner_ref, trans_ref, cyc_ref,
           own, colp, rowp, inb, mask, acc, sendbuf, recvbuf,
           load_sem, x_send, own_send, y_send, relay_send, col_recv, in_send, in_recv,
           up_send, dn_send, sib_send, row_recv, res_send, res_recv):
    rb, cb = out_ref.shape
    tr, ct = rb // TILE, cb // TILE
    nt, slots = list_ref.shape
    lines, ys = cols_n // 2, rows_n // 2
    reach = sendbuf.shape[0]
    hb = rb // HALVES
    me_r, me_c = lax.axis_index("row"), lax.axis_index("col")
    yy, p = me_r // 2, me_r % 2
    zz, a = me_c // 2, me_c % 2
    vr, vc = 2 * yy + a, 2 * zz + p

    def home(r, c):
        return (2 * (r // 2) + c % 2, 2 * (c // 2) + r % 2)

    load = pltpu.make_async_copy(out_ref, own, load_sem)
    load.start()

    barrier = pltpu.get_barrier_semaphore()

    def greet(i, carry):
        there = (me_r + i // 2) % rows_n, 2 * zz + (a + i % 2) % 2
        pl.semaphore_signal(barrier, inc=1, device_id=there, device_id_type=MESH)
        return carry

    above, below = (me_c + 2) % cols_n, (me_c + cols_n - 2) % cols_n
    pl.semaphore_signal(barrier, inc=1, device_id=(me_r, above), device_id_type=MESH)
    pl.semaphore_signal(barrier, inc=1, device_id=(me_r, below), device_id_type=MESH)
    lax.fori_loop(1, rows_n * 2, greet, 0)
    load.wait()
    pl.semaphore_wait(barrier, rows_n * 2 + 1)

    def half(h):
        return pl.ds(h * hb, hb)

    def col_at(group, h):
        return colp.at[pl.ds(pl.multiple_of(group * rb + h * hb, hb), hb)]

    def send(src, dst, send_sem, recv_sem, there):
        return pltpu.make_async_remote_copy(
            src_ref=src, dst_ref=dst, send_sem=send_sem, recv_sem=recv_sem, device_id=there, device_id_type=MESH)

    sibling = (2 * yy + 1 - p, me_c)
    across = (2 * yy + a, 2 * zz + 1 - a)

    def over_x(h):
        return send(own.at[half(h)], col_at(me_r, h), x_send.at[h], col_recv.at[me_r, h], across)

    def to_sibling(h):
        return send(own.at[half(h)], col_at(me_r, h), own_send.at[h], col_recv.at[me_r, h], sibling)

    def keep(h):
        return pltpu.make_async_copy(own.at[half(h)], col_at(me_r, h), col_recv.at[me_r, h])

    def over_y(d, h):
        there = (2 * ((yy + d) % ys) + a, me_c)
        return send(own.at[half(h)], col_at(me_r, h), y_send.at[d, h], col_recv.at[me_r, h], there)

    def relay(group, b, d, h):
        there = (2 * ((yy + d) % ys) + p, me_c)
        return send(col_at(group, h), col_at(group, h), relay_send.at[b, d, h], col_recv.at[group, h], there)

    def wait_col(group, h):
        pltpu.make_async_copy(col_at(group, h), col_at(group, h), col_recv.at[group, h]).wait()

    give_in = send(in_ref, inb, in_send, in_recv, across)
    keep_in = pltpu.make_async_copy(in_ref, inb, in_recv)

    @pl.when(a == p)
    def _():
        for h in range(HALVES):
            keep(h).start()

    @pl.when(a != p)
    def _():
        for h in range(HALVES):
            over_x(h).start()

    def start_y():
        for d in range(1, ys):
            for h in range(HALVES):
                over_y(d, h).start()

    @pl.when(a != p)
    def _():
        start_y()
        for h in range(HALVES):
            to_sibling(h).start()

    def up(slot, h, src):
        return send(src, rowp.at[slot, half(h)], up_send.at[slot, h], row_recv.at[slot, h], (me_r, above))

    def down(slot, h, src):
        return send(src, rowp.at[slot, half(h)], dn_send.at[slot, h], row_recv.at[slot, h], (me_r, below))

    def sib(slot, h, src):
        return send(src, rowp.at[slot, half(h)], sib_send.at[slot, h], row_recv.at[slot, h], sibling)

    def wait_row(slot, h):
        pltpu.make_async_copy(rowp.at[slot, half(h)], rowp.at[slot, half(h)], row_recv.at[slot, h]).wait()

    far = lines // 2

    def low_of(d):
        return 2 * ((zz + lines - d) % lines) + p

    def high_of(d):
        return 2 * ((zz + d) % lines) + p

    def goes_up(d, h):
        return d < far or (d == far and h == 0)

    def goes_down(d, h):
        return d < far or (d == far and h == 1)

    for h in range(HALVES):
        wait_col(vr, h)
        if goes_up(1, h):
            up(vc, h, col_at(vr, h)).start()
        if goes_down(1, h):
            down(vc, h, col_at(vr, h)).start()
        sib(vc, h, col_at(vr, h)).start()

    @pl.when(a == p)
    def _():
        start_y()

    @pl.when(a != p)
    def _():
        give_in.start()
        for d in range(1, ys):
            for h in range(HALVES):
                relay(vr, 0, d, h).start()

    @pl.when(a == p)
    def _():
        keep_in.start()

    row_ids = lax.broadcasted_iota(jnp.int32, (nt, TILE), 0)
    lane_ids = lax.broadcasted_iota(jnp.int32, (nt, TILE), 1)
    counts = lax.fori_loop(
        0, nt, lambda t, c: jnp.where(row_ids == t, count_ref[t], c), jnp.zeros((nt, TILE), jnp.int32))
    small = jnp.zeros((nt, TILE), jnp.float32)
    for s in range(slots):
        hit = (list_ref[:, s:s + 1] == lane_ids) & (counts > s)
        small = jnp.where(hit, 1.0, small)

    def spread(t, carry):
        one = jnp.sum(jnp.where(lane_ids == t, small, 0.0), axis=1, keepdims=True)
        mask[t] = jnp.broadcast_to(one, (nt, TILE))
        return carry

    lax.fori_loop(0, nt, spread, 0)

    def forward(d):
        for h in range(HALVES):
            if goes_up(d, h):
                slot = low_of(d)
                wait_row(slot, h)
                if goes_up(d + 1, h):
                    up(slot, h, rowp.at[slot, half(h)]).start()
                sib(slot, h, rowp.at[slot, half(h)]).start()
            if goes_down(d, h):
                slot = high_of(d)
                wait_row(slot, h)
                if goes_down(d + 1, h):
                    down(slot, h, rowp.at[slot, half(h)]).start()
                sib(slot, h, rowp.at[slot, half(h)]).start()
            if d == 1 and h == 0:
                @pl.when(a == p)
                def _():
                    for k in range(HALVES):
                        over_x(k).start()

    def keep_of(tile, column):
        wide = [mask[column * ct + j, pl.ds(tile, 1), :] for j in range(ct)]
        return jnp.concatenate(wide, axis=1)

    def tiles(block, first_tile, column):
        parts = []
        for t in range(block.shape[0] // TILE):
            keep = keep_of(first_tile + t, column)
            parts.append(block[t * TILE:(t + 1) * TILE] * keep.astype(jnp.bfloat16))
        return jnp.concatenate(parts, axis=0)

    def product(slot, lhs):
        left = tiles(lhs, tr * vr, slot)
        right = tiles(colp[pl.ds(pl.multiple_of(slot * cb, cb), cb), :], ct * slot, vc)
        return jnp.dot(left, right, preferred_element_type=jnp.float32)

    def add(slot):
        acc[...] += product(slot, rowp[slot])

    def take(slot):
        add(slot)
        for h in range(HALVES):
            wait_row(slot + 1 - 2 * p, h)
        add(slot + 1 - 2 * p)

    other = 2 * yy + 1 - a
    forward(1)

    @pl.when(a != p)
    def _():
        for h in range(HALVES):
            wait_col(other, h)
            for d in range(1, ys):
                relay(other, 1, d, h).start()

    @pl.when(a == p)
    def _():
        for h in range(HALVES):
            wait_col(other, h)

    for d in range(2, far):
        forward(d)

    def wait_cols(i, carry):
        for h in range(HALVES):
            wait_col((2 * yy + i) % rows_n, h)
        return carry

    if far > 1:
        forward(far)
    lax.fori_loop(2, rows_n, wait_cols, 0)
    acc[...] = product(vc, colp[pl.ds(pl.multiple_of(vr * rb, rb), rb), :])
    for h in range(HALVES):
        wait_row(vc + 1 - 2 * p, h)
    add(vc + 1 - 2 * p)

    def take_both(d, carry):
        take(low_of(d))
        take(high_of(d))
        return carry

    lax.fori_loop(1, far, take_both, 0)
    take(low_of(far))
    keep_in.wait()

    lefts, rights = [], []
    for q in range(tr):
        at = pl.ds(pl.multiple_of(vr * rb + q * TILE, TILE), TILE)
        total = acc[q * TILE:(q + 1) * TILE, :]
        keep = keep_of(tr * vr + q, vc)
        t_prod = colp[at, :].astype(jnp.float32) * keep * total
        t_sum, c_sum = 0.0, 0.0
        for j in range(ct):
            cols = slice(j * TILE, (j + 1) * TILE)
            keep_in_tile = mask[tr * vr + q, pl.ds(ct * vc + j, 1), :]
            t_sum += t_prod[:, cols]
            c_sum += inb[q * TILE:(q + 1) * TILE, cols].astype(jnp.float32) * keep_in_tile * total[:, cols]
        lefts.append(jnp.sum(t_sum.T, axis=0, keepdims=True))
        rights.append(jnp.sum(c_sum.T, axis=0, keepdims=True))
    for e in range(reach):
        dest = (vr + e) % rows_n
        t_out, c_out = jnp.zeros((1, TILE), jnp.float32), jnp.zeros((1, TILE), jnp.float32)
        for q in range(tr):
            mine = owner_ref[tr * vr + q] == dest
            t_out = jnp.where(mine, lefts[q], t_out)
            c_out = jnp.where(mine, rights[q], c_out)
        sendbuf[e, 0:1, :] = t_out
        sendbuf[e, 1:2, :] = c_out

    def result(e, i):
        return pltpu.make_async_remote_copy(
            src_ref=sendbuf.at[e], dst_ref=recvbuf.at[e, vc], send_sem=res_send.at[e, i],
            recv_sem=res_recv, device_id=((vr + e) % rows_n, (me_c + i) % cols_n), device_id_type=MESH)

    def each_result(act, act_here):
        for e in range(reach):
            def one(i, carry, e=e):
                here = ((vr + e) % rows_n == me_r) & (i == 0)
                pl.when(jnp.logical_not(here))(lambda: act(result(e, i)))
                return carry

            lax.fori_loop(0, cols_n, one, 0)
            if act_here:
                @pl.when((vr + e) % rows_n == me_r)
                def _():
                    pltpu.make_async_copy(sendbuf.at[e], recvbuf.at[e, vc], res_recv).start()

    each_result(lambda c: c.start(), True)

    @pl.when(a != p)
    def _():
        give_in.wait_send()
        for h in range(HALVES):
            to_sibling(h).wait_send()
            for d in range(1, ys):
                relay(vr, 0, d, h).wait_send()
                relay(other, 1, d, h).wait_send()

    for h in range(HALVES):
        over_x(h).wait_send()
        for d in range(1, ys):
            over_y(d, h).wait_send()

    for d in range(far + 1):
        for h in range(HALVES):
            low, high = low_of(d), high_of(d)
            if goes_up(d, h):
                if goes_up(d + 1, h):
                    up(low, h, rowp.at[low, half(h)]).wait_send()
                sib(low, h, rowp.at[low, half(h)]).wait_send()
            if goes_down(d, h):
                if goes_down(d + 1, h):
                    down(high, h, rowp.at[high, half(h)]).wait_send()
                if d > 0:
                    sib(high, h, rowp.at[high, half(h)]).wait_send()
    each_result(lambda c: c.wait_send(), False)

    pltpu.make_async_copy(recvbuf, recvbuf, res_recv).wait()
    for e in range(reach):
        group = (me_r + rows_n - e) % rows_n
        place = 0
        for other in range(reach):
            place += ((me_r + rows_n - other) % rows_n < group).astype(jnp.int32)
        both = jnp.sum(recvbuf[e], axis=0)
        at = pl.ds(pl.multiple_of(place * TILE, TILE), TILE)
        trans_ref[at] = both[0]
        cyc_ref[at] = both[1]


def solution(mesh):
    rows_n, cols_n = mesh.shape["row"], mesh.shape["col"]

    def per_device(out_weights, in_weights, tile_list, tile_count, owner):
        rb, cb = out_weights.shape
        nt = tile_list.shape[0]
        tr = rb // TILE
        lines = cols_n // 2
        assert rows_n % 2 == 0 and lines % 2 == 0 and lines > 2 and tr <= rows_n
        n = rows_n * rb
        block = pltpu.VMEM((rb, cb), out_weights.dtype)
        dma = pltpu.SemaphoreType.DMA
        any_space = pl.BlockSpec(memory_space=pl.ANY)
        vmem = pl.BlockSpec(memory_space=pltpu.VMEM)
        smem = pl.BlockSpec(memory_space=pltpu.SMEM)
        trans, cyc = pl.pallas_call(
            functools.partial(kernel, rows_n, cols_n),
            out_shape=[jax.ShapeDtypeStruct((rb,), jnp.float32)] * 2,
            in_specs=[any_space, any_space, vmem, smem, smem],
            out_specs=[vmem, vmem],
            scratch_shapes=[
                block,
                pltpu.VMEM((n, cb), out_weights.dtype),
                pltpu.VMEM((cols_n, rb, cb), out_weights.dtype),
                block,
                pltpu.VMEM((nt, nt, TILE), jnp.float32),
                pltpu.VMEM((rb, cb), jnp.float32),
                pltpu.VMEM((tr, 2, TILE), jnp.float32),
                pltpu.VMEM((tr, cols_n, 2, TILE), jnp.float32),
                dma, dma((HALVES,)), dma((HALVES,)),
                dma((rows_n // 2, HALVES)), dma((2, rows_n // 2, HALVES)), dma((rows_n, HALVES)),
                dma, dma,
                dma((cols_n, HALVES)), dma((cols_n, HALVES)), dma((cols_n, HALVES)), dma((cols_n, HALVES)),
                dma((tr, cols_n)), dma,
            ],
            compiler_params=pltpu.CompilerParams(collective_id=0, has_side_effects=True),
            name="census",
        )(out_weights, in_weights, tile_list, tile_count, owner)
        return trans, cyc

    return jax.shard_map(
        per_device, mesh=mesh,
        in_specs=(P("row", "col"), P("row", "col"), P(), P(), P()),
        out_specs=(P("row"), P("row")), check_vma=False)
```

```python
import functools

import jax
import jax.numpy as jnp
from jax import lax
from jax.experimental import pallas as pl
from jax.experimental.pallas import tpu as pltpu
from jax.sharding import PartitionSpec as P

TILE = 128
HALVES = 2
MESH = pl.DeviceIdType.MESH


def kernel(rows_n, cols_n, out_ref, in_ref, list_ref, count_ref, owner_ref, trans_ref, cyc_ref,
           own, colp, rowp, inb, mask, acc, sendbuf, recvbuf,
           load_sem, x_send, own_send, y_send, relay_send, col_recv, in_send, in_recv,
           up_send, dn_send, sib_send, row_recv, res_send, res_recv):
    rb, cb = out_ref.shape
    tr, ct = rb // TILE, cb // TILE
    nt, slots = list_ref.shape
    lines, ys = cols_n // 2, rows_n // 2
    reach = sendbuf.shape[0]
    hb = rb // HALVES
    me_r, me_c = lax.axis_index("row"), lax.axis_index("col")
    yy, p = me_r // 2, me_r % 2
    zz, a = me_c // 2, me_c % 2
    vr, vc = 2 * yy + a, 2 * zz + p

    def home(r, c):
        return (2 * (r // 2) + c % 2, 2 * (c // 2) + r % 2)

    load = pltpu.make_async_copy(out_ref, own, load_sem)
    load.start()

    barrier = pltpu.get_barrier_semaphore()

    def greet(i, carry):
        there = (me_r + i // 2) % rows_n, 2 * zz + (a + i % 2) % 2
        pl.semaphore_signal(barrier, inc=1, device_id=there, device_id_type=MESH)
        return carry

    above, below = me_c + 2, me_c - 2
    has_above, has_below = zz < lines - 1, zz > 0

    @pl.when(has_above)
    def _():
        pl.semaphore_signal(barrier, inc=1, device_id=(me_r, above), device_id_type=MESH)

    @pl.when(has_below)
    def _():
        pl.semaphore_signal(barrier, inc=1, device_id=(me_r, below), device_id_type=MESH)

    lax.fori_loop(1, rows_n * 2, greet, 0)
    load.wait()
    expected = rows_n * 2 - 1 + has_above.astype(jnp.int32) + has_below.astype(jnp.int32)
    pl.semaphore_wait(barrier, expected)

    def half(h):
        return pl.ds(h * hb, hb)

    def col_at(group, h):
        return colp.at[pl.ds(pl.multiple_of(group * rb + h * hb, hb), hb)]

    def send(src, dst, send_sem, recv_sem, there):
        return pltpu.make_async_remote_copy(
            src_ref=src, dst_ref=dst, send_sem=send_sem, recv_sem=recv_sem, device_id=there, device_id_type=MESH)

    sibling = (2 * yy + 1 - p, me_c)
    across = (2 * yy + a, 2 * zz + 1 - a)

    def over_x(h):
        return send(own.at[half(h)], col_at(me_r, h), x_send.at[h], col_recv.at[me_r, h], across)

    def to_sibling(h):
        return send(own.at[half(h)], col_at(me_r, h), own_send.at[h], col_recv.at[me_r, h], sibling)

    def keep(h):
        return pltpu.make_async_copy(own.at[half(h)], col_at(me_r, h), col_recv.at[me_r, h])

    def over_y(d, h):
        there = (2 * ((yy + d) % ys) + a, me_c)
        return send(own.at[half(h)], col_at(me_r, h), y_send.at[d, h], col_recv.at[me_r, h], there)

    def relay(group, b, d, h):
        there = (2 * ((yy + d) % ys) + p, me_c)
        return send(col_at(group, h), col_at(group, h), relay_send.at[b, d, h], col_recv.at[group, h], there)

    def wait_col(group, h):
        pltpu.make_async_copy(col_at(group, h), col_at(group, h), col_recv.at[group, h]).wait()

    give_in = send(in_ref, inb, in_send, in_recv, across)
    keep_in = pltpu.make_async_copy(in_ref, inb, in_recv)

    @pl.when(a == p)
    def _():
        for h in range(HALVES):
            keep(h).start()

    @pl.when(a != p)
    def _():
        for h in range(HALVES):
            over_x(h).start()

    def start_y():
        for d in range(1, ys):
            for h in range(HALVES):
                over_y(d, h).start()

    @pl.when(a != p)
    def _():
        start_y()
        for h in range(HALVES):
            to_sibling(h).start()

    def up(slot, h, src):
        return send(src, rowp.at[slot, half(h)], up_send.at[slot, h], row_recv.at[slot, h], (me_r, above))

    def down(slot, h, src):
        return send(src, rowp.at[slot, half(h)], dn_send.at[slot, h], row_recv.at[slot, h], (me_r, below))

    def sib(slot, h, src):
        return send(src, rowp.at[slot, half(h)], sib_send.at[slot, h], row_recv.at[slot, h], sibling)

    def wait_row(slot, h):
        pltpu.make_async_copy(rowp.at[slot, half(h)], rowp.at[slot, half(h)], row_recv.at[slot, h]).wait()

    for h in range(HALVES):
        wait_col(vr, h)
        pl.when(has_above)(lambda h=h: up(vc, h, col_at(vr, h)).start())
        pl.when(has_below)(lambda h=h: down(vc, h, col_at(vr, h)).start())
        sib(vc, h, col_at(vr, h)).start()

    @pl.when(a == p)
    def _():
        start_y()

    @pl.when(a != p)
    def _():
        give_in.start()
        for d in range(1, ys):
            for h in range(HALVES):
                relay(vr, 0, d, h).start()

    @pl.when(a == p)
    def _():
        keep_in.start()

    row_ids = lax.broadcasted_iota(jnp.int32, (nt, TILE), 0)
    lane_ids = lax.broadcasted_iota(jnp.int32, (nt, TILE), 1)
    counts = lax.fori_loop(
        0, nt, lambda t, c: jnp.where(row_ids == t, count_ref[t], c), jnp.zeros((nt, TILE), jnp.int32))
    small = jnp.zeros((nt, TILE), jnp.float32)
    for s in range(slots):
        hit = (list_ref[:, s:s + 1] == lane_ids) & (counts > s)
        small = jnp.where(hit, 1.0, small)

    def spread(t, carry):
        one = jnp.sum(jnp.where(lane_ids == t, small, 0.0), axis=1, keepdims=True)
        mask[t] = jnp.broadcast_to(one, (nt, TILE))
        return carry

    lax.fori_loop(0, nt, spread, 0)

    def low_of(d):
        return 2 * (zz - d) + p

    def high_of(d):
        return 2 * (zz + d) + p

    def forward(d):
        for h in range(HALVES):
            @pl.when(zz - d >= 0)
            def _():
                slot = low_of(d)
                wait_row(slot, h)
                pl.when(has_above)(lambda: up(slot, h, rowp.at[slot, half(h)]).start())
                sib(slot, h, rowp.at[slot, half(h)]).start()

            @pl.when(zz + d < lines)
            def _():
                slot = high_of(d)
                wait_row(slot, h)
                pl.when(has_below)(lambda: down(slot, h, rowp.at[slot, half(h)]).start())
                sib(slot, h, rowp.at[slot, half(h)]).start()

    def keep_of(tile, column):
        wide = [mask[column * ct + j, pl.ds(tile, 1), :] for j in range(ct)]
        return jnp.concatenate(wide, axis=1)

    def tiles(block, first_tile, column):
        parts = []
        for t in range(block.shape[0] // TILE):
            keep = keep_of(first_tile + t, column)
            parts.append(block[t * TILE:(t + 1) * TILE] * keep.astype(jnp.bfloat16))
        return jnp.concatenate(parts, axis=0)

    def product(slot, lhs):
        left = tiles(lhs, tr * vr, slot)
        right = tiles(colp[pl.ds(pl.multiple_of(slot * cb, cb), cb), :], ct * slot, vc)
        return jnp.dot(left, right, preferred_element_type=jnp.float32)

    def add(slot):
        acc[...] += product(slot, rowp[slot])

    def take(slot):
        add(slot)
        for h in range(HALVES):
            wait_row(slot + 1 - 2 * p, h)
        add(slot + 1 - 2 * p)

    other = 2 * yy + 1 - a
    forward(1)

    @pl.when(a == p)
    def _():
        for h in range(HALVES):
            over_x(h).start()

    @pl.when(a != p)
    def _():
        for h in range(HALVES):
            wait_col(other, h)
            for d in range(1, ys):
                relay(other, 1, d, h).start()

    @pl.when(a == p)
    def _():
        for h in range(HALVES):
            wait_col(other, h)

    lax.fori_loop(2, lines - 1, lambda d, c: (forward(d), c)[1], 0)

    def wait_cols(i, carry):
        for h in range(HALVES):
            wait_col((2 * yy + i) % rows_n, h)
        return carry

    lax.fori_loop(2, rows_n, wait_cols, 0)
    acc[...] = product(vc, colp[pl.ds(pl.multiple_of(vr * rb, rb), rb), :])
    for h in range(HALVES):
        wait_row(vc + 1 - 2 * p, h)
    add(vc + 1 - 2 * p)

    def take_both(d):
        pl.when(zz - d >= 0)(lambda: take(low_of(d)))
        pl.when(zz + d < lines)(lambda: take(high_of(d)))

    lax.fori_loop(1, lines - 1, lambda d, c: (take_both(d), c)[1], 0)
    keep_in.wait()
    forward(lines - 1)
    take_both(lines - 1)

    lefts, rights = [], []
    for q in range(tr):
        at = pl.ds(pl.multiple_of(vr * rb + q * TILE, TILE), TILE)
        total = acc[q * TILE:(q + 1) * TILE, :]
        keep = keep_of(tr * vr + q, vc)
        t_prod = colp[at, :].astype(jnp.float32) * keep * total
        t_sum, c_sum = 0.0, 0.0
        for j in range(ct):
            cols = slice(j * TILE, (j + 1) * TILE)
            keep_in_tile = mask[tr * vr + q, pl.ds(ct * vc + j, 1), :]
            t_sum += t_prod[:, cols]
            c_sum += inb[q * TILE:(q + 1) * TILE, cols].astype(jnp.float32) * keep_in_tile * total[:, cols]
        lefts.append(jnp.sum(t_sum.T, axis=0, keepdims=True))
        rights.append(jnp.sum(c_sum.T, axis=0, keepdims=True))
    for e in range(reach):
        dest = (vr + e) % rows_n
        t_out, c_out = jnp.zeros((1, TILE), jnp.float32), jnp.zeros((1, TILE), jnp.float32)
        for q in range(tr):
            mine = owner_ref[tr * vr + q] == dest
            t_out = jnp.where(mine, lefts[q], t_out)
            c_out = jnp.where(mine, rights[q], c_out)
        sendbuf[e, 0:1, :] = t_out
        sendbuf[e, 1:2, :] = c_out

    def result(e, i):
        return pltpu.make_async_remote_copy(
            src_ref=sendbuf.at[e], dst_ref=recvbuf.at[e, vc], send_sem=res_send.at[e, i],
            recv_sem=res_recv, device_id=((vr + e) % rows_n, (me_c + i) % cols_n), device_id_type=MESH)

    def each_result(act, act_here):
        for e in range(reach):
            def one(i, carry, e=e):
                here = ((vr + e) % rows_n == me_r) & (i == 0)
                pl.when(jnp.logical_not(here))(lambda: act(result(e, i)))
                return carry

            lax.fori_loop(0, cols_n, one, 0)
            if act_here:
                @pl.when((vr + e) % rows_n == me_r)
                def _():
                    pltpu.make_async_copy(sendbuf.at[e], recvbuf.at[e, vc], res_recv).start()

    each_result(lambda c: c.start(), True)

    @pl.when(a != p)
    def _():
        give_in.wait_send()
        for h in range(HALVES):
            to_sibling(h).wait_send()
            for d in range(1, ys):
                relay(vr, 0, d, h).wait_send()
                relay(other, 1, d, h).wait_send()

    for h in range(HALVES):
        over_x(h).wait_send()
        for d in range(1, ys):
            over_y(d, h).wait_send()

    def drain(d, carry):
        for h in range(HALVES):
            low, high = low_of(d), high_of(d)

            @pl.when(zz - d >= 0)
            def _():
                pl.when(has_above)(lambda: up(low, h, rowp.at[low, half(h)]).wait_send())
                sib(low, h, rowp.at[low, half(h)]).wait_send()

            @pl.when(zz + d < lines)
            def _():
                pl.when(has_below)(lambda: down(high, h, rowp.at[high, half(h)]).wait_send())
                pl.when(d > 0)(lambda: sib(high, h, rowp.at[high, half(h)]).wait_send())
        return carry

    lax.fori_loop(0, lines, drain, 0)
    each_result(lambda c: c.wait_send(), False)

    pltpu.make_async_copy(recvbuf, recvbuf, res_recv).wait()
    for e in range(reach):
        group = (me_r + rows_n - e) % rows_n
        place = 0
        for other in range(reach):
            place += ((me_r + rows_n - other) % rows_n < group).astype(jnp.int32)
        both = jnp.sum(recvbuf[e], axis=0)
        at = pl.ds(pl.multiple_of(place * TILE, TILE), TILE)
        trans_ref[at] = both[0]
        cyc_ref[at] = both[1]


def solution(mesh):
    rows_n, cols_n = mesh.shape["row"], mesh.shape["col"]

    def per_device(out_weights, in_weights, tile_list, tile_count, owner):
        rb, cb = out_weights.shape
        nt = tile_list.shape[0]
        tr = rb // TILE
        lines = cols_n // 2
        assert rows_n % 2 == 0 and cols_n % 2 == 0 and tr <= rows_n
        n = rows_n * rb
        block = pltpu.VMEM((rb, cb), out_weights.dtype)
        dma = pltpu.SemaphoreType.DMA
        any_space = pl.BlockSpec(memory_space=pl.ANY)
        vmem = pl.BlockSpec(memory_space=pltpu.VMEM)
        smem = pl.BlockSpec(memory_space=pltpu.SMEM)
        trans, cyc = pl.pallas_call(
            functools.partial(kernel, rows_n, cols_n),
            out_shape=[jax.ShapeDtypeStruct((rb,), jnp.float32)] * 2,
            in_specs=[any_space, any_space, vmem, smem, smem],
            out_specs=[vmem, vmem],
            scratch_shapes=[
                block,
                pltpu.VMEM((n, cb), out_weights.dtype),
                pltpu.VMEM((cols_n, rb, cb), out_weights.dtype),
                block,
                pltpu.VMEM((nt, nt, TILE), jnp.float32),
                pltpu.VMEM((rb, cb), jnp.float32),
                pltpu.VMEM((tr, 2, TILE), jnp.float32),
                pltpu.VMEM((tr, cols_n, 2, TILE), jnp.float32),
                dma, dma((HALVES,)), dma((HALVES,)),
                dma((rows_n // 2, HALVES)), dma((2, rows_n // 2, HALVES)), dma((rows_n, HALVES)),
                dma, dma,
                dma((cols_n, HALVES)), dma((cols_n, HALVES)), dma((cols_n, HALVES)), dma((cols_n, HALVES)),
                dma((tr, cols_n)), dma,
            ],
            compiler_params=pltpu.CompilerParams(collective_id=0, has_side_effects=True),
            name="census",
        )(out_weights, in_weights, tile_list, tile_count, owner)
        def last(t_in, c_in, t_out, c_out):
            t_out[...] = t_in[...]
            c_out[...] = c_in[...]

        return pl.pallas_call(
            last, out_shape=[jax.ShapeDtypeStruct((rb,), jnp.float32)] * 2,
            in_specs=[vmem, vmem], out_specs=[vmem, vmem], name="last")(trans, cyc)

    return jax.shard_map(
        per_device, mesh=mesh,
        in_specs=(P("row", "col"), P("row", "col"), P(), P(), P()),
        out_specs=(P("row"), P("row")), check_vma=False)
```

```python
import functools

import jax
import jax.numpy as jnp
from jax import lax
from jax.experimental import pallas as pl
from jax.experimental.pallas import tpu as pltpu
from jax.sharding import PartitionSpec as P

TILE = 128
HALVES = 2
MESH = pl.DeviceIdType.MESH


def kernel(rows_n, cols_n, out_ref, in_ref, list_ref, count_ref, owner_ref, trans_ref, cyc_ref,
           own, colp, rowp, inb, mask, acc, sendbuf, recvbuf,
           load_sem, x_send, own_send, y_send, relay_send, col_recv, in_send, in_recv,
           up_send, dn_send, sib_send, row_recv, res_send, res_recv):
    rb, cb = out_ref.shape
    tr, ct = rb // TILE, cb // TILE
    nt, slots = list_ref.shape
    lines, ys = cols_n // 2, rows_n // 2
    reach = sendbuf.shape[0]
    hb = rb // HALVES
    me_r, me_c = lax.axis_index("row"), lax.axis_index("col")
    yy, p = me_r // 2, me_r % 2
    zz, a = me_c // 2, me_c % 2
    vr, vc = 2 * yy + a, 2 * zz + p

    def home(r, c):
        return (2 * (r // 2) + c % 2, 2 * (c // 2) + r % 2)

    load = pltpu.make_async_copy(out_ref, own, load_sem)
    load.start()

    barrier = pltpu.get_barrier_semaphore()

    def greet(i, carry):
        there = (me_r + i // 2) % rows_n, 2 * zz + (a + i % 2) % 2
        pl.semaphore_signal(barrier, inc=1, device_id=there, device_id_type=MESH)
        return carry

    above, below = me_c + 2, me_c - 2
    has_above, has_below = zz < lines - 1, zz > 0

    @pl.when(has_above)
    def _():
        pl.semaphore_signal(barrier, inc=1, device_id=(me_r, above), device_id_type=MESH)

    @pl.when(has_below)
    def _():
        pl.semaphore_signal(barrier, inc=1, device_id=(me_r, below), device_id_type=MESH)

    lax.fori_loop(1, rows_n * 2, greet, 0)
    row_ids = lax.broadcasted_iota(jnp.int32, (nt, TILE), 0)
    lane_ids = lax.broadcasted_iota(jnp.int32, (nt, TILE), 1)
    counts = lax.fori_loop(
        0, nt, lambda t, c: jnp.where(row_ids == t, count_ref[t], c), jnp.zeros((nt, TILE), jnp.int32))
    small = jnp.zeros((nt, TILE), jnp.float32)
    for s in range(slots):
        hit = (list_ref[:, s:s + 1] == lane_ids) & (counts > s)
        small = jnp.where(hit, 1.0, small)

    def spread(t, carry):
        one = jnp.sum(jnp.where(lane_ids == t, small, 0.0), axis=1, keepdims=True)
        mask[t] = jnp.broadcast_to(one, (nt, TILE))
        return carry

    lax.fori_loop(0, nt, spread, 0)

    load.wait()
    expected = rows_n * 2 - 1 + has_above.astype(jnp.int32) + has_below.astype(jnp.int32)
    pl.semaphore_wait(barrier, expected)

    def half(h):
        return pl.ds(h * hb, hb)

    def col_at(group, h):
        return colp.at[pl.ds(pl.multiple_of(group * rb + h * hb, hb), hb)]

    def send(src, dst, send_sem, recv_sem, there):
        return pltpu.make_async_remote_copy(
            src_ref=src, dst_ref=dst, send_sem=send_sem, recv_sem=recv_sem, device_id=there, device_id_type=MESH)

    sibling = (2 * yy + 1 - p, me_c)
    across = (2 * yy + a, 2 * zz + 1 - a)

    def over_x(h):
        return send(own.at[half(h)], col_at(me_r, h), x_send.at[h], col_recv.at[me_r, h], across)

    def to_sibling(h):
        return send(own.at[half(h)], col_at(me_r, h), own_send.at[h], col_recv.at[me_r, h], sibling)

    def keep(h):
        return pltpu.make_async_copy(own.at[half(h)], col_at(me_r, h), col_recv.at[me_r, h])

    def over_y(d, h):
        there = (2 * ((yy + d) % ys) + a, me_c)
        return send(own.at[half(h)], col_at(me_r, h), y_send.at[d, h], col_recv.at[me_r, h], there)

    def relay(group, b, d, h):
        there = (2 * ((yy + d) % ys) + p, me_c)
        return send(col_at(group, h), col_at(group, h), relay_send.at[b, d, h], col_recv.at[group, h], there)

    def wait_col(group, h):
        pltpu.make_async_copy(col_at(group, h), col_at(group, h), col_recv.at[group, h]).wait()

    give_in = send(in_ref, inb, in_send, in_recv, across)
    keep_in = pltpu.make_async_copy(in_ref, inb, in_recv)

    @pl.when(a == p)
    def _():
        for h in range(HALVES):
            keep(h).start()

    @pl.when(a != p)
    def _():
        for h in range(HALVES):
            over_x(h).start()

    def start_y():
        for d in range(1, ys):
            for h in range(HALVES):
                over_y(d, h).start()

    @pl.when(a != p)
    def _():
        start_y()
        for h in range(HALVES):
            to_sibling(h).start()

    def up(slot, h, src):
        return send(src, rowp.at[slot, half(h)], up_send.at[slot, h], row_recv.at[slot, h], (me_r, above))

    def down(slot, h, src):
        return send(src, rowp.at[slot, half(h)], dn_send.at[slot, h], row_recv.at[slot, h], (me_r, below))

    def sib(slot, h, src):
        return send(src, rowp.at[slot, half(h)], sib_send.at[slot, h], row_recv.at[slot, h], sibling)

    def wait_row(slot, h):
        pltpu.make_async_copy(rowp.at[slot, half(h)], rowp.at[slot, half(h)], row_recv.at[slot, h]).wait()

    for h in range(HALVES):
        wait_col(vr, h)
        pl.when(has_above)(lambda h=h: up(vc, h, col_at(vr, h)).start())
        pl.when(has_below)(lambda h=h: down(vc, h, col_at(vr, h)).start())
        sib(vc, h, col_at(vr, h)).start()

    @pl.when(a == p)
    def _():
        start_y()

    @pl.when(a != p)
    def _():
        give_in.start()
        for d in range(1, ys):
            for h in range(HALVES):
                relay(vr, 0, d, h).start()

    @pl.when(a == p)
    def _():
        keep_in.start()

    def low_of(d):
        return 2 * (zz - d) + p

    def high_of(d):
        return 2 * (zz + d) + p

    def forward(d):
        for h in range(HALVES):
            @pl.when(zz - d >= 0)
            def _():
                slot = low_of(d)
                wait_row(slot, h)
                pl.when(has_above)(lambda: up(slot, h, rowp.at[slot, half(h)]).start())
                sib(slot, h, rowp.at[slot, half(h)]).start()

            @pl.when(zz + d < lines)
            def _():
                slot = high_of(d)
                wait_row(slot, h)
                pl.when(has_below)(lambda: down(slot, h, rowp.at[slot, half(h)]).start())
                sib(slot, h, rowp.at[slot, half(h)]).start()

    def keep_of(tile, column):
        wide = [mask[column * ct + j, pl.ds(tile, 1), :] for j in range(ct)]
        return jnp.concatenate(wide, axis=1)

    def tiles(block, first_tile, column):
        parts = []
        for t in range(block.shape[0] // TILE):
            keep = keep_of(first_tile + t, column)
            parts.append(block[t * TILE:(t + 1) * TILE] * keep.astype(jnp.bfloat16))
        return jnp.concatenate(parts, axis=0)

    def product(slot, lhs):
        left = tiles(lhs, tr * vr, slot)
        right = tiles(colp[pl.ds(pl.multiple_of(slot * cb, cb), cb), :], ct * slot, vc)
        return jnp.dot(left, right, preferred_element_type=jnp.float32)

    def add(slot):
        acc[...] += product(slot, rowp[slot])

    def take(slot):
        add(slot)
        for h in range(HALVES):
            wait_row(slot + 1 - 2 * p, h)
        add(slot + 1 - 2 * p)

    other = 2 * yy + 1 - a
    forward(1)

    @pl.when(a == p)
    def _():
        for h in range(HALVES):
            over_x(h).start()

    @pl.when(a != p)
    def _():
        for h in range(HALVES):
            wait_col(other, h)
            for d in range(1, ys):
                relay(other, 1, d, h).start()

    @pl.when(a == p)
    def _():
        for h in range(HALVES):
            wait_col(other, h)

    lax.fori_loop(2, lines - 1, lambda d, c: (forward(d), c)[1], 0)

    def wait_cols(i, carry):
        for h in range(HALVES):
            wait_col((2 * yy + i) % rows_n, h)
        return carry

    lax.fori_loop(2, rows_n, wait_cols, 0)
    acc[...] = product(vc, colp[pl.ds(pl.multiple_of(vr * rb, rb), rb), :])
    for h in range(HALVES):
        wait_row(vc + 1 - 2 * p, h)
    add(vc + 1 - 2 * p)

    def take_both(d):
        pl.when(zz - d >= 0)(lambda: take(low_of(d)))
        pl.when(zz + d < lines)(lambda: take(high_of(d)))

    lax.fori_loop(1, lines - 1, lambda d, c: (take_both(d), c)[1], 0)
    keep_in.wait()
    forward(lines - 1)
    take_both(lines - 1)

    lefts, rights = [], []
    for q in range(tr):
        at = pl.ds(pl.multiple_of(vr * rb + q * TILE, TILE), TILE)
        total = acc[q * TILE:(q + 1) * TILE, :]
        keep = keep_of(tr * vr + q, vc)
        t_prod = colp[at, :].astype(jnp.float32) * keep * total
        t_sum, c_sum = 0.0, 0.0
        for j in range(ct):
            cols = slice(j * TILE, (j + 1) * TILE)
            keep_in_tile = mask[tr * vr + q, pl.ds(ct * vc + j, 1), :]
            t_sum += t_prod[:, cols]
            c_sum += inb[q * TILE:(q + 1) * TILE, cols].astype(jnp.float32) * keep_in_tile * total[:, cols]
        lefts.append(jnp.sum(t_sum.T, axis=0, keepdims=True))
        rights.append(jnp.sum(c_sum.T, axis=0, keepdims=True))
    for e in range(reach):
        dest = (vr + e) % rows_n
        t_out, c_out = jnp.zeros((1, TILE), jnp.float32), jnp.zeros((1, TILE), jnp.float32)
        for q in range(tr):
            mine = owner_ref[tr * vr + q] == dest
            t_out = jnp.where(mine, lefts[q], t_out)
            c_out = jnp.where(mine, rights[q], c_out)
        sendbuf[e, 0:1, :] = t_out
        sendbuf[e, 1:2, :] = c_out

    def result(e, i):
        return pltpu.make_async_remote_copy(
            src_ref=sendbuf.at[e], dst_ref=recvbuf.at[e, vc], send_sem=res_send.at[e, i],
            recv_sem=res_recv, device_id=((vr + e) % rows_n, (me_c + i) % cols_n), device_id_type=MESH)

    def each_result(act, act_here):
        for e in range(reach):
            def one(i, carry, e=e):
                here = ((vr + e) % rows_n == me_r) & (i == 0)
                pl.when(jnp.logical_not(here))(lambda: act(result(e, i)))
                return carry

            lax.fori_loop(0, cols_n, one, 0)
            if act_here:
                @pl.when((vr + e) % rows_n == me_r)
                def _():
                    pltpu.make_async_copy(sendbuf.at[e], recvbuf.at[e, vc], res_recv).start()

    each_result(lambda c: c.start(), True)

    @pl.when(a != p)
    def _():
        give_in.wait_send()
        for h in range(HALVES):
            to_sibling(h).wait_send()
            for d in range(1, ys):
                relay(vr, 0, d, h).wait_send()
                relay(other, 1, d, h).wait_send()

    for h in range(HALVES):
        over_x(h).wait_send()
        for d in range(1, ys):
            over_y(d, h).wait_send()

    def drain(d, carry):
        for h in range(HALVES):
            low, high = low_of(d), high_of(d)

            @pl.when(zz - d >= 0)
            def _():
                pl.when(has_above)(lambda: up(low, h, rowp.at[low, half(h)]).wait_send())
                sib(low, h, rowp.at[low, half(h)]).wait_send()

            @pl.when(zz + d < lines)
            def _():
                pl.when(has_below)(lambda: down(high, h, rowp.at[high, half(h)]).wait_send())
                pl.when(d > 0)(lambda: sib(high, h, rowp.at[high, half(h)]).wait_send())
        return carry

    lax.fori_loop(0, lines, drain, 0)
    each_result(lambda c: c.wait_send(), False)

    pltpu.make_async_copy(recvbuf, recvbuf, res_recv).wait()
    for e in range(reach):
        group = (me_r + rows_n - e) % rows_n
        place = 0
        for other in range(reach):
            place += ((me_r + rows_n - other) % rows_n < group).astype(jnp.int32)
        both = jnp.sum(recvbuf[e], axis=0)
        at = pl.ds(pl.multiple_of(place * TILE, TILE), TILE)
        trans_ref[at] = both[0]
        cyc_ref[at] = both[1]


def solution(mesh):
    rows_n, cols_n = mesh.shape["row"], mesh.shape["col"]

    def per_device(out_weights, in_weights, tile_list, tile_count, owner):
        rb, cb = out_weights.shape
        nt = tile_list.shape[0]
        tr = rb // TILE
        lines = cols_n // 2
        assert rows_n % 2 == 0 and cols_n % 2 == 0 and tr <= rows_n
        n = rows_n * rb
        block = pltpu.VMEM((rb, cb), out_weights.dtype)
        dma = pltpu.SemaphoreType.DMA
        any_space = pl.BlockSpec(memory_space=pl.ANY)
        vmem = pl.BlockSpec(memory_space=pltpu.VMEM)
        smem = pl.BlockSpec(memory_space=pltpu.SMEM)
        trans, cyc = pl.pallas_call(
            functools.partial(kernel, rows_n, cols_n),
            out_shape=[jax.ShapeDtypeStruct((rb,), jnp.float32)] * 2,
            in_specs=[any_space, any_space, vmem, smem, smem],
            out_specs=[vmem, vmem],
            scratch_shapes=[
                block,
                pltpu.VMEM((n, cb), out_weights.dtype),
                pltpu.VMEM((cols_n, rb, cb), out_weights.dtype),
                block,
                pltpu.VMEM((nt, nt, TILE), jnp.float32),
                pltpu.VMEM((rb, cb), jnp.float32),
                pltpu.VMEM((tr, 2, TILE), jnp.float32),
                pltpu.VMEM((tr, cols_n, 2, TILE), jnp.float32),
                dma, dma((HALVES,)), dma((HALVES,)),
                dma((rows_n // 2, HALVES)), dma((2, rows_n // 2, HALVES)), dma((rows_n, HALVES)),
                dma, dma,
                dma((cols_n, HALVES)), dma((cols_n, HALVES)), dma((cols_n, HALVES)), dma((cols_n, HALVES)),
                dma((tr, cols_n)), dma,
            ],
            compiler_params=pltpu.CompilerParams(collective_id=0, has_side_effects=True),
            name="census",
        )(out_weights, in_weights, tile_list, tile_count, owner)
        def last(t_in, c_in, t_out, c_out):
            t_out[...] = t_in[...]
            c_out[...] = c_in[...]

        return pl.pallas_call(
            last, out_shape=[jax.ShapeDtypeStruct((rb,), jnp.float32)] * 2,
            in_specs=[vmem, vmem], out_specs=[vmem, vmem], name="last")(trans, cyc)

    return jax.shard_map(
        per_device, mesh=mesh,
        in_specs=(P("row", "col"), P("row", "col"), P(), P(), P()),
        out_specs=(P("row"), P("row")), check_vma=False)
```
